32 devices in a mesh: vocab: 8 (over z, y), dp: 4 (over x, core).
Axes of the slice: x: 2, y: 2, z: 4, core: 2. Of those that a mesh axis runs over, the one named last changes fastest.
Arguments:
- hidden: bfloat16 [4096, 4096], P('dp'), may hold values from -6 to 6
- labels: int32 [4096], P('dp'), may hold values from 0 to 3, as said below
- targets: int32 [4096], P('dp'), may hold values from 0 to 147455, as said below
- head_weight: bfloat16 [4096, 16384], P(None, 'vocab'), may hold values from -0.125 to 0.125
- cluster_weight: bfloat16 [4096, 3], replicated, may hold values from -0.09375 to 0.09375
- proj_one: bfloat16 [4096, 1024], P('vocab'), may hold values from -0.09375 to 0.09375
- proj_two: bfloat16 [4096, 256], P('vocab'), may hold values from -0.09375 to 0.09375
- proj_three: bfloat16 [4096, 64], P('vocab'), may hold values from -0.09375 to 0.09375
- out_one: bfloat16 [1024, 32768], P(None, 'vocab'), may hold values from -0.1875 to 0.1875
- out_two: bfloat16 [256, 65536], P(None, 'vocab'), may hold values from -0.375 to 0.375
- out_three: bfloat16 [64, 147456], P(None, 'vocab'), may hold values from -0.75 to 0.75
Outputs:
- token_loss: float32 [4096], P('dp')
- mean_loss: float32 [], replicated
- hidden_grad: float32 [4096, 4096], P('dp', 'vocab')
The draws below stay inside these ranges and needn't reach their ends.
Inputs may be any that keep to these rules, and one draw needn't show every extreme that they name: In each aligned block of 1024 tokens (one index of dp), each of the labels 1, 2 and 3 marks at most 256 tokens and at least 128; for each label some block holds exactly 256 of them. `targets`: A token's target is below 16384 if its label is 0, below 32768, 65536 or 147456 if its label is 1, 2 or 3.
All inputs are finite; a program needn't handle non-finite values.
Results may differ from the reference program's by a relative error of at most 0.0013.
Values sent between devices are 32-bit elements; how exact they have to be, the bound alone decides.
A program may use at most 128 MiB of HBM per device.

```python
import jax
import jax.numpy as jnp
from jax import lax

D = 4096
HEAD = 16384
P1 = 1024
P2 = 256
P3 = 64
V1 = 32768
V2 = 65536
V3 = 147456
GRP_TOK = 1024
CAP = 256
TOKENS = 4096


def label_parts(key):
    groups = TOKENS // GRP_TOK
    first_key, second_key, third_key, fourth_key = jax.random.split(jax.random.fold_in(key, 17), 4)
    full_group = jax.random.randint(first_key, (3,), 0, groups)
    amounts = jax.random.randint(second_key, (groups, 3), CAP // 2, CAP + 1)
    amounts = jnp.where(jnp.arange(groups)[:, None] == full_group[None, :], CAP, amounts).astype(jnp.int32)
    edges = jnp.cumsum(amounts, axis=1)
    places = jnp.arange(GRP_TOK, dtype=jnp.int32)[None, :]
    sorted_labels = jnp.where(places < edges[:, 0:1], 1, jnp.where(places < edges[:, 1:2], 2, jnp.where(places < edges[:, 2:3], 3, 0)))
    shuffles = jax.vmap(lambda sub_key: jax.random.permutation(sub_key, GRP_TOK))(jax.random.split(third_key, groups))
    labels = jnp.take_along_axis(sorted_labels, shuffles, axis=1).reshape(TOKENS).astype(jnp.int32)
    limits = jnp.array([HEAD, V1, V2, V3], jnp.int32)[labels]
    raw_ids = jax.random.randint(fourth_key, (TOKENS,), 0, 2 ** 30, dtype=jnp.int32)
    targets = (raw_ids % limits).astype(jnp.int32)
    return (labels, targets)


def draw_labels(key, part):
    return label_parts(key)[0]


def draw_targets(key, part):
    return label_parts(key)[1]


def raised(values, own_key, source, target, shards_of, factor):
    owner, partner = [(jnp.arange(values.shape[axis_at]) // (values.shape[axis_at] // shards_of)).reshape([-1 if axis == axis_at else 1 for axis in range(values.ndim)]) for axis_at in (source, target)]
    chosen = jax.random.permutation(own_key, shards_of)[partner]
    strong = (owner == chosen) | (owner == (partner + shards_of // 2) % shards_of)
    return jnp.where(strong, factor * values, values)


def levels(key, extent, pieces, smallest, largest):
    loudness = 1.0
    for position, shards_of in pieces:
        steps = jax.random.uniform(jax.random.fold_in(jax.random.fold_in(key, 6), position), (shards_of,), jnp.float32, smallest / len(pieces), largest / len(pieces))
        loudness = loudness * jnp.repeat(jnp.exp(steps), extent[position] // shards_of).reshape((-1,) + (1,) * (len(extent) - 1 - position))
    return loudness


def gaussian(key, extent, deviation, most, cuts=(), kind=jnp.bfloat16):
    factor_of = levels(key, extent, cuts, -0.22, 0.18) if cuts else 1.0
    values = jax.random.normal(key, extent, jnp.float32) * deviation * factor_of
    return jnp.minimum(jnp.maximum(values, -most), most).astype(kind)


def bell_draw_with(key, extent, width, reach, shards, heavy, kind=jnp.bfloat16):
    values = width * jax.random.normal(key, extent, jnp.float32)
    if shards:
        values = values * levels(key, extent, shards, -0.22, 0.18)
    return jnp.clip(raised(values, jax.random.fold_in(key, 3), *heavy), -reach, reach).astype(kind)


def setup_inputs(seed: int = 0) -> dict:
    streams_of = jax.random.split(jax.random.key(seed), 12)
    hidden = gaussian(streams_of[0], (TOKENS, D), 1.0, 6.0, ((0, 4),))
    labels = draw_labels(jax.random.fold_in(streams_of[11], 71), 0)
    targets = draw_targets(jax.random.fold_in(streams_of[11], 71), 0)
    head_weight = bell_draw_with(streams_of[3], (D, HEAD), D ** -0.5, 0.125, ((1, 8),), (1, 0, 8, 2.0))
    cluster_weight = gaussian(streams_of[4], (D, 3), D ** -0.5, 0.09375)
    proj_one = gaussian(streams_of[5], (D, P1), D ** -0.5, 0.09375, ((0, 8),))
    proj_two = gaussian(streams_of[6], (D, P2), D ** -0.5, 0.09375, ((0, 8),))
    proj_three = gaussian(streams_of[7], (D, P3), D ** -0.5, 0.09375, ((0, 8),))
    out_one = gaussian(streams_of[8], (P1, V1), P1 ** -0.5, 0.1875, ((1, 8),))
    out_two = gaussian(streams_of[9], (P2, V2), P2 ** -0.5, 0.375, ((1, 8),))
    out_three = gaussian(streams_of[10], (P3, V3), P3 ** -0.5, 0.75, ((1, 8),))
    return {"hidden": hidden, "labels": labels, "targets": targets, "head_weight": head_weight, "cluster_weight": cluster_weight, "proj_one": proj_one, "proj_two": proj_two, "proj_three": proj_three, "out_one": out_one, "out_two": out_two, "out_three": out_three}


capping = 30.0

def capped(values):
    return capping * jnp.tanh(values / capping)

def cluster_slots(labels, cluster, capacity):
    member = labels == cluster
    placed = jnp.cumsum(member.astype(jnp.int32)) - 1
    slot_of = jnp.where(member, placed, capacity).astype(jnp.int32)
    order = jnp.arange(labels.shape[0], dtype=jnp.int32)
    slot_rows = jnp.zeros((capacity + 1,), jnp.int32).at[slot_of].set(order)[:capacity]
    filled = (jnp.arange(capacity, dtype=jnp.int32) < jnp.sum(member.astype(jnp.int32))).astype(jnp.float32)
    return (slot_rows, filled)

def reference(hidden, labels, targets, head_weight, cluster_weight, proj_one, proj_two, proj_three, out_one, out_two, out_three):
    groups = TOKENS // GRP_TOK
    capacity = GRP_TOK // 4
    factor = jnp.sqrt(jnp.float32(D))
    tails = ((proj_one, out_one), (proj_two, out_two), (proj_three, out_three))
    counts = jnp.stack([jnp.sum((labels == cluster).astype(jnp.float32)) for cluster in (1, 2, 3)])
    weights = TOKENS / (4.0 * counts)

    def group_terms(packed):
        rows, labs, aims = packed
        head_cap = capped(jnp.dot(rows, head_weight, preferred_element_type=jnp.float32))
        clus_cap = capped(jnp.dot(rows, cluster_weight, preferred_element_type=jnp.float32))
        head_exp = jnp.exp(head_cap)
        clus_exp = jnp.exp(clus_cap)
        total = lax.optimization_barrier(jnp.sum(head_exp, 1)) + lax.optimization_barrier(jnp.sum(clus_exp, 1))
        head_hit = ((labs == 0)[:, None] & (jnp.arange(HEAD, dtype=jnp.int32)[None, :] == aims[:, None])).astype(jnp.float32)
        clus_hit = (jnp.arange(3, dtype=jnp.int32)[None, :] + 1 == labs[:, None]).astype(jnp.float32)
        picked = lax.optimization_barrier(jnp.sum(head_hit * head_cap, 1)) + lax.optimization_barrier(jnp.sum(clus_hit * clus_cap, 1))
        token_loss = jnp.log(total) - picked
        head_grad = (factor * (head_exp / total[:, None] - head_hit) * (1.0 - (head_cap / capping) ** 2)).astype(jnp.bfloat16)
        clus_grad = factor * (clus_exp / total[:, None] - clus_hit) * (1.0 - (clus_cap / capping) ** 2)
        grads = jnp.dot(head_grad, head_weight.T, preferred_element_type=jnp.float32)
        grads = grads + jnp.dot(clus_grad, cluster_weight.astype(jnp.float32).T, precision=lax.Precision.HIGHEST)
        for number in range(3):
            proj, out = tails[number]
            slot_rows, filled = cluster_slots(labs, number + 1, capacity)
            latent = jnp.dot(rows[slot_rows], proj, preferred_element_type=jnp.float32)
            tail_cap = capped(jnp.dot(latent, out.astype(jnp.float32), precision=lax.Precision.HIGHEST))
            tail_exp = jnp.exp(tail_cap)
            tail_total = lax.optimization_barrier(jnp.sum(tail_exp, 1))
            tail_hit = (jnp.arange(out.shape[1], dtype=jnp.int32)[None, :] == aims[slot_rows][:, None]).astype(jnp.float32) * filled[:, None]
            tail_loss = (jnp.log(tail_total) - lax.optimization_barrier(jnp.sum(tail_hit * tail_cap, 1))) * filled
            tail_grad = (factor * (tail_exp / tail_total[:, None] - tail_hit) * (1.0 - (tail_cap / capping) ** 2) * filled[:, None]).astype(jnp.bfloat16)
            latent_grad = jnp.dot(tail_grad, out.T, preferred_element_type=jnp.float32)
            back = jnp.dot(latent_grad, proj.astype(jnp.float32).T, precision=lax.Precision.HIGHEST)
            token_loss = token_loss.at[slot_rows].add(weights[number] * tail_loss)
            grads = grads.at[slot_rows].add(weights[number] * back)
        return (token_loss, grads)
    losses, grads = lax.map(group_terms, (hidden.reshape(groups, GRP_TOK, D), labels.reshape(groups, GRP_TOK), targets.reshape(groups, GRP_TOK)))
    token_loss = losses.reshape(TOKENS)
    mean_loss = jnp.sum(token_loss) / TOKENS
    return (token_loss, mean_loss, grads.reshape(TOKENS, D))
```

```python
import functools

import jax
import jax.numpy as jnp
from jax import lax
from jax.sharding import PartitionSpec as P


capping = 30.0
RING_LIMIT = 16
STREAMS = 2


def capped(values):
    return capping * jnp.tanh(values * (1.0 / capping))


def butterfly_sum(values, axis, n):
    step = 1
    while step < n:
        pairs = [(i, i ^ step) for i in range(n)]
        other = lax.ppermute(values, axis, pairs)
        values = values + other
        step *= 2
    return values


def halving_sum(values, axis, n, steps):
    me = lax.axis_index(axis)
    bits = []
    for step in steps:
        bit = (me // step) % 2
        pairs = [(i, i ^ step) for i in range(n)]
        half = values.shape[0] // 2
        send = lax.dynamic_slice_in_dim(values, (1 - bit) * half, half, 0)
        keep = lax.dynamic_slice_in_dim(values, bit * half, half, 0)
        values = keep + lax.ppermute(send, axis, pairs)
        bits.append((bit, pairs))
    for bit, pairs in reversed(bits):
        other = lax.ppermute(values, axis, pairs)
        first = bit == 0
        values = jnp.concatenate(
            [jnp.where(first, values, other), jnp.where(first, other, values)], 0
        )
    return values


def ring_scatter(grad, weight, axis, n, width):
    order = list(range(0, n, 2)) + list(range(n - 1, 0, -2))
    place = [0] * n
    for position, index in enumerate(order):
        place[index] = position
    me = lax.axis_index(axis)
    position = jnp.asarray(place, jnp.int32)[me]
    blocks = jnp.asarray(order, jnp.int32)
    rows = grad.shape[0] // STREAMS
    ways = []
    for stream in range(STREAMS):
        part = lax.slice_in_dim(grad, stream * rows, (stream + 1) * rows, axis=0)
        sign = 1 if stream % 2 == 0 else -1
        pairs = [(order[i], order[(i + sign) % n]) for i in range(n)]
        ways.append((part, sign, pairs))

    def term(part, sign, hop):
        block = blocks[(position - sign * (1 + hop) + 2 * n) % n]
        own = lax.dynamic_slice_in_dim(weight, block * width, width, 0)
        return jnp.einsum("tv,fv->tf", part, own, preferred_element_type=jnp.float32)

    held = [term(part, sign, 0) for part, sign, _ in ways]
    for hop in range(1, n):
        for i, (part, sign, pairs) in enumerate(ways):
            came = lax.ppermute(held[i], axis, pairs)
            came, part = lax.optimization_barrier((came, part))
            held[i] = came + term(part, sign, hop)
    return jnp.concatenate(held, 0)


def per_device(
    n,
    groups,
    hidden,
    labels,
    targets,
    head_weight,
    cluster_weight,
    proj_one,
    proj_two,
    proj_three,
    out_one,
    out_two,
    out_three,
):
    f32, bf16 = jnp.float32, jnp.bfloat16
    tokens = hidden.shape[0]
    width = proj_one.shape[0]
    head_local = head_weight.shape[1]
    capacity = tokens // 4
    all_tokens = tokens * groups
    vocab_index = lax.axis_index("vocab")
    feat_start = vocab_index * width
    factor = jnp.sqrt(f32(hidden.shape[1]))
    projs = (proj_one, proj_two, proj_three)
    outs = (out_one, out_two, out_three)

    member = labels[None, :] == jnp.arange(1, 4, dtype=jnp.int32)[:, None]
    local_counts = jnp.sum(member.astype(f32), 1)
    row = jnp.arange(tokens, dtype=jnp.int32)
    upto = (row[:, None] <= row[None, :]).astype(bf16)
    placed = jnp.dot(member.astype(bf16), upto, preferred_element_type=f32).astype(jnp.int32) - 1
    offsets = jnp.arange(3, dtype=jnp.int32)[:, None] * capacity
    slot_of = jnp.sum(jnp.where(member, placed + offsets + 1, 0), 0) - 1
    slot_ids = jnp.arange(3 * capacity, dtype=jnp.int32)
    chosen = slot_ids[:, None] == slot_of[None, :]
    select = chosen.astype(bf16)
    slot_aims = jnp.sum(jnp.where(chosen, targets[None, :] + 1, 0), 1) - 1
    filled = (slot_aims >= 0).astype(f32)

    own_features = lax.dynamic_slice_in_dim(hidden, feat_start, width, 1)
    picked_rows = jnp.dot(select, own_features, preferred_element_type=f32).astype(bf16)
    latent_parts = []
    for number in range(3):
        chunk = picked_rows[number * capacity : (number + 1) * capacity]
        latent_parts.append(jnp.dot(chunk, projs[number], preferred_element_type=f32))
    powers = []
    step = 1
    while step < n:
        powers.append(step)
        step *= 2
    turned = powers[1:] + powers[:1]
    joined = jnp.concatenate([latent_parts[1], latent_parts[2]], 1)
    joined = halving_sum(joined, "vocab", n, turned)
    width_two = projs[1].shape[1]
    latents = [
        halving_sum(latent_parts[0], "vocab", n, powers),
        joined[:, :width_two],
        joined[:, width_two:],
    ]
    counts = butterfly_sum(local_counts, "dp", groups)
    weights = all_tokens / (4.0 * counts)

    head_cap = capped(jnp.dot(hidden, head_weight, preferred_element_type=f32))
    head_sum = jnp.sum(jnp.exp(head_cap), 1)
    head_sum = butterfly_sum(head_sum, "vocab", n)
    clus_cap = capped(jnp.dot(hidden, cluster_weight, preferred_element_type=f32))
    clus_exp = jnp.exp(clus_cap)
    clus_hit = (jnp.arange(3, dtype=jnp.int32)[None, :] + 1 == labels[:, None]).astype(f32)
    head_aims = jnp.where(labels == 0, targets, -1) - vocab_index * head_local
    head_hit = jnp.arange(head_local, dtype=jnp.int32)[None, :] == head_aims[:, None]
    total = head_sum + jnp.sum(clus_exp, 1)
    scale = factor / total
    kept_cap = lax.optimization_barrier(head_cap)
    head_pick = jnp.sum(jnp.where(head_hit, kept_cap, 0.0), 1)
    slope = 1.0 - (kept_cap * (1.0 / capping)) ** 2
    head_grad = (
        (jnp.exp(kept_cap) * scale[:, None] - jnp.where(head_hit, factor, 0.0)) * slope
    ).astype(bf16)
    clus_grad = (clus_exp * scale[:, None] - factor * clus_hit) * (
        1.0 - (clus_cap * (1.0 / capping)) ** 2
    )
    if n <= RING_LIMIT:
        head_back = ring_scatter(head_grad, head_weight, "vocab", n, width)
    else:
        head_terms = jnp.einsum("tv,fv->tf", head_grad, head_weight, preferred_element_type=f32)
        head_back = lax.psum_scatter(head_terms, "vocab", scatter_dimension=1, tiled=True)

    tail_caps, tail_hits, tail_sums, tail_picks = [None] * 3, [None] * 3, [None] * 3, [None] * 3
    for number in (1, 2, 0):
        out = outs[number]
        tail_cap = capped(
            jnp.dot(latents[number], out.astype(f32), precision=lax.Precision.HIGH)
        )
        aims = slot_aims[number * capacity : (number + 1) * capacity]
        aims = jnp.where(aims >= 0, aims, -1) - vocab_index * out.shape[1]
        aims = jnp.where(slot_aims[number * capacity : (number + 1) * capacity] >= 0, aims, -1)
        tail_hits[number] = jnp.arange(out.shape[1], dtype=jnp.int32)[None, :] == aims[:, None]
        tail_sums[number] = jnp.sum(jnp.exp(tail_cap), 1)
        tail_caps[number] = lax.optimization_barrier(tail_cap)
        tail_picks[number] = jnp.sum(jnp.where(tail_hits[number], tail_caps[number], 0.0), 1)
    tail_totals = butterfly_sum(jnp.concatenate(tail_sums), "vocab", n)
    tail_scales = factor * filled / tail_totals
    grad_parts = [None] * 3
    for number in (0, 1, 2):
        cap = tail_caps[number]
        tail_scale = tail_scales[number * capacity : (number + 1) * capacity]
        tail_grad = (
            (jnp.exp(cap) * tail_scale[:, None] - jnp.where(tail_hits[number], factor, 0.0))
            * (1.0 - (cap * (1.0 / capping)) ** 2)
        ).astype(bf16)
        grad_parts[number] = jnp.einsum(
            "sv,pv->sp", tail_grad, outs[number], preferred_element_type=f32
        )
    grad_one = halving_sum(grad_parts[0], "vocab", n, powers)
    grad_rest = halving_sum(jnp.concatenate([grad_parts[1], grad_parts[2]], 1), "vocab", n, turned)
    latent_grads = [grad_one, grad_rest[:, :width_two], grad_rest[:, width_two:]]

    backs = []
    for number in range(3):
        back = jnp.einsum(
            "sp,fp->sf",
            latent_grads[number],
            projs[number].astype(f32),
            precision=lax.Precision.HIGH,
        )
        backs.append(weights[number] * back)
    back = jnp.concatenate(backs, 0)
    back_top = lax.reduce_precision(back, 8, 7)
    back_rest = (back - back_top).astype(bf16)
    back_top = back_top.astype(bf16)
    pick_slots = functools.partial(jnp.einsum, "st,sf->tf", preferred_element_type=f32)
    tail_back = pick_slots(select, back_top) + pick_slots(select, back_rest)
    clus_rows = lax.dynamic_slice_in_dim(cluster_weight, feat_start, width, 0).astype(f32)
    clus_back = (
        clus_grad[:, 0:1] * clus_rows[:, 0][None, :]
        + clus_grad[:, 1:2] * clus_rows[:, 1][None, :]
        + clus_grad[:, 2:3] * clus_rows[:, 2][None, :]
    )
    grads = head_back + (tail_back + clus_back)

    picks = butterfly_sum(jnp.concatenate([head_pick] + tail_picks), "vocab", n)
    head_loss = jnp.log(total) - picks[:tokens] - jnp.sum(clus_hit * clus_cap, 1)
    tail_loss = (jnp.log(tail_totals) - picks[tokens:]) * filled
    slot_weights = jnp.repeat(weights, capacity)
    tail_loss = tail_loss * slot_weights
    token_loss = head_loss + jnp.sum(jnp.where(chosen, tail_loss[:, None], 0.0), 0)
    loss_sum = butterfly_sum(jnp.sum(token_loss)[None], "dp", groups)
    mean_loss = loss_sum[0] / all_tokens
    return (token_loss, mean_loss, grads)


def solution(mesh):
    body = functools.partial(per_device, mesh.shape["vocab"], mesh.shape["dp"])
    return jax.shard_map(
        body,
        mesh=mesh,
        in_specs=(
            P("dp", None),
            P("dp"),
            P("dp"),
            P(None, "vocab"),
            P(),
            P("vocab", None),
            P("vocab", None),
            P("vocab", None),
            P(None, "vocab"),
            P(None, "vocab"),
            P(None, "vocab"),
        ),
        out_specs=(P("dp"), P(), P("dp", "vocab")),
        check_vma=False,
    )
```
